32 devices in a mesh: cell: 4 (over z), wide: 8 (over y, x, core).
Axes of the slice: x: 2, y: 2, z: 4, core: 2. Of those that a mesh axis runs over, the one named last changes fastest.
Arguments:
- positions: float32 [3, 4, 64, 128], P(None, 'cell', 'wide'), may hold values from 0 to 1
- rhs: float32 [3, 4, 64, 128], P(None, 'cell', 'wide'), may hold values from -6 to 6
- blob_owner: int32 [4, 64, 128, 1], P('cell', 'wide'), may hold values from 0 to 31; in each aligned block of 1024 rows (0 to 1023, 1024 to 2047, ..., all dimensions but the last counted through in order) at most 128 rows name the same one
- blob_row: int32 [4, 64, 128], P('cell', 'wide'), may hold values from 0 to 31
- blob_arm: float32 [3, 4, 64, 128], P(None, 'cell', 'wide'), may hold values from -1 to 1
- body_inverse: float32 [6, 6, 1024], P(None, None, ('cell', 'wide'))
Outputs:
- blob_forces: float32 [3, 4, 64, 128], P(None, 'cell', 'wide')
- body_motion: float32 [6, 1024], P(None, ('cell', 'wide'))
The draws below stay inside these ranges and needn't reach their ends.
Inputs may be any that keep to these rules, and one draw needn't show every extreme that they name: `blob_owner`: at most 128 of the blobs of one device have bodies of one owner, and that many in some device.
All inputs are finite; a program needn't handle non-finite values.
Results may differ from the reference program's by a relative error of at most 0.0003.
Values sent between devices are 32-bit elements; how exact they have to be, the bound alone decides.
A program may use at most 64 MiB of HBM per device.

```python
import math
import jax
import jax.numpy as jnp
import numpy as np
from jax import lax

TILE = 128
NEIGH = 9
ITERS = 3
TY = 8
BODY_DEV = 32
GX = 4
GY = 64
BLOB_DEV = 1024
NBODY = 1024
BLOB_BODY = 32
CAP = 128
N_CELL = 4
N_WIDE = 8
DEVICES = 32


def draw_body_inverse(key, part):
    first, second = jax.random.split(jax.random.fold_in(key, 23))
    noise = jax.random.normal(first, (6, 6, NBODY), jnp.float32) * 0.15
    symmetric = 0.5 * (noise + jnp.transpose(noise, (1, 0, 2)))
    scales = jnp.exp(jax.random.uniform(second, (NBODY,), jnp.float32, 0.0, math.log(4.0))) / BLOB_BODY
    unit = jnp.eye(6, dtype=jnp.float32)[:, :, None]
    return ((unit + symmetric) * scales[None, None]).astype(jnp.float32)


def plant(drawn, stream_key, smallest, largest):
    shape = drawn.shape
    spot = [jax.random.randint(jax.random.fold_in(stream_key, axis), (), 0, shape[axis]) for axis in range(len(shape))]
    drawn = drawn.at[tuple(spot)].set(smallest)
    longest = shape.index(max(shape))
    spot[longest] = (spot[longest] + 1) % shape[longest]
    return drawn.at[tuple(spot)].set(largest)


def steps_of(stream_key, dims, pieces, least, high):
    gain, own = 1.0, jax.random.fold_in(stream_key, 6)
    for position, blocks in pieces:
        steps = jnp.exp(jax.random.uniform(jax.random.fold_in(own, position), (blocks,), jnp.float32, least / len(pieces), high / len(pieces)))
        gain = gain * jnp.repeat(steps, dims[position] // blocks).reshape([-1 if axis == position else 1 for axis in range(len(dims))])
    return gain


def assign_block(own_key, own, number, rows, amount, top, most, lean):
    ranking = jax.random.permutation(own_key, amount)
    crowded, usual = shares(amount, rows * top, most, lean, True), shares(amount, rows * top, most, lean, False)
    places = jnp.arange(amount)

    def named(tallies, turn):
        used = int((tallies > 0).sum())
        fixed = max(1, used // 4)
        moved = fixed + (places - fixed + turn * (used - fixed)) % max(1, amount - fixed)
        return jnp.zeros((amount,), jnp.int32).at[ranking[jnp.where(places < fixed, places, moved)]].set(jnp.asarray(tallies, jnp.int32))

    tallies = jnp.where(number % 4 == 0, named(crowded, number // 4), named(usual, number - number // 4 - 1))
    mixed = jax.random.permutation(jax.random.fold_in(own, 3), amount)
    giver, taker = mixed[0:amount // 2 * 2:2], mixed[1:amount // 2 * 2:2]
    slack = jnp.minimum(tallies[giver] - 1, most - tallies[taker]) // 2
    slack = jnp.where((giver == ranking[0]) | (taker == ranking[0]) | (tallies[taker] == 0), 0, jnp.maximum(slack, 0))
    moved = jax.random.randint(jax.random.fold_in(own, 4), (amount // 2,), 0, 1 << 20) % (slack + 1)
    tallies = tallies.at[giver].add(-moved).at[taker].add(moved)
    items = jnp.searchsorted(jnp.cumsum(tallies), jnp.arange(rows * top), side="right").astype(jnp.int32)
    grid = items.reshape(top, rows).T
    grid = grid[jax.random.permutation(jax.random.fold_in(own, 1), rows)]
    turn = jax.random.randint(jax.random.fold_in(own, 2), (rows, 1), 0, top)
    return jnp.take_along_axis(grid, (jnp.arange(top)[None, :] + turn) % top, axis=1)


def shares(count, total, limit, skew, full):
    loads = [(1 << 20) // math.isqrt(rank ** skew) + 1 for rank in range(1, count + 1)]
    largest = limit if full else min(limit, max(-(-total // count), total * loads[0] // sum(loads)))
    least = 1 if total - largest >= count - 1 else 0
    counts, spare = [largest] + [least] * (count - 1), total - largest - least * (count - 1)
    while spare > 0:
        candidates = [i for i in range(1, count) if counts[i] < largest] or [i for i in range(1, count) if counts[i] < limit]
        pool, left = sum([loads[i] for i in candidates]), spare
        for i in candidates:
            more = min(limit - counts[i], max(1, left * loads[i] // pool), spare)
            counts[i] = counts[i] + more
            spare = spare - more
    return np.array(counts)


def scatter_about(own_key, extent, width, limit, cuts=(), kind=jnp.bfloat16):
    values = jax.random.normal(own_key, extent, jnp.float32) * width
    if len(cuts) > 0:
        values = steps_of(own_key, extent, cuts, -0.22, 0.18) * values
    return jnp.clip(values, min=-limit, max=limit).astype(kind)


def setup_inputs(seed: int = 0) -> dict:
    streams_of = jax.random.split(jax.random.key(seed), 7)
    positions = jnp.clip(1.0 * jax.random.uniform(streams_of[0], (3, GX, GY, TILE), jnp.float32) ** steps_of(streams_of[0], (3, GX, GY, TILE), ((1, 4), (2, 8)), -0.2, 0.2), 0.0, 1.0)
    rhs = scatter_about(streams_of[1], (3, GX, GY, TILE), 1.0, 6.0, ((1, 4), (2, 8)), jnp.float32)
    blob_owner_keys = jax.random.split(jax.random.fold_in(streams_of[2], 1), GX * GY * TILE // BLOB_DEV)
    blob_owner_turns = jax.random.permutation(jax.random.fold_in(streams_of[2], 3), GX * GY * TILE // BLOB_DEV)
    blob_owner = jax.vmap(lambda own, number: assign_block(jax.random.fold_in(streams_of[2], 2), own, number, BLOB_DEV, DEVICES, 1, CAP, 2))(blob_owner_keys, blob_owner_turns).reshape((GX, GY, TILE, 1))
    blob_row = plant(jax.random.randint(streams_of[3], (GX, GY, TILE), 0, BODY_DEV), jax.random.fold_in(streams_of[3], 1), 0, BODY_DEV - 1).astype(jnp.int32)
    blob_arm = jnp.clip(jax.random.uniform(streams_of[4], (3, GX, GY, TILE), jnp.float32, -1.0, 1.0) * steps_of(streams_of[4], (3, GX, GY, TILE), ((1, 4), (2, 8)), -0.4, 0.0), -1.0, 1.0)
    body_inverse = draw_body_inverse(jax.random.fold_in(streams_of[6], 71), 0)
    return {"positions": positions, "rhs": rhs, "blob_owner": blob_owner, "blob_row": blob_row, "blob_arm": blob_arm, "body_inverse": body_inverse}


EPS2 = 0.04
KAPPA = 0.3

def pair_sum(target, source, forces):
    sep = target[..., :, None] - source[..., None, :]
    dist2 = lax.optimization_barrier(jnp.sum(sep * sep, axis=0))
    soft = dist2 + EPS2
    inverse = 1.0 / (soft * jnp.sqrt(soft))
    near = (dist2 + 2.0 * EPS2) * inverse
    along = lax.optimization_barrier(jnp.sum(sep * forces[..., None, :], axis=0))
    return lax.optimization_barrier(jnp.sum(near[None] * forces[..., None, :] + (inverse * along)[None] * sep, axis=-1))

def shifted(field, code, with_offset):
    step_x = code // 3 - 1
    step_y = code % 3 - 1
    moved = jnp.roll(field, (-step_x, -step_y), axis=(1, 2))
    if with_offset:
        moved = moved + jnp.array([step_x, step_y, 0], jnp.float32)[:, None, None, None]
    return moved

def blocks(field):
    return jnp.moveaxis(field.reshape(3, N_CELL * N_WIDE, TY, TILE), 1, 0)

def mobility(field, positions):
    total = jnp.zeros_like(field)
    for code in range(NEIGH):
        source = shifted(positions, code, True)
        forces = shifted(field, code, False)
        part = lax.map(lambda item: pair_sum(item[0], item[1], item[2]), (blocks(positions), blocks(source), blocks(forces)))
        total = total + jnp.moveaxis(part, 0, 1).reshape(field.shape)
    return field + KAPPA / math.sqrt(NEIGH * TILE) * total

def precondition(field, arms, body_ids, body_inverse):
    values = field.reshape(3, -1)
    sent = jnp.concatenate([values, jnp.cross(arms, values, axis=0)], 0)
    sums = jax.ops.segment_sum(sent.T, body_ids, num_segments=NBODY).T
    motion = jnp.einsum('abn,bn->an', body_inverse, sums, precision=lax.Precision.HIGHEST)
    back = motion[:, body_ids]
    extra = back[:3] + jnp.cross(back[3:], arms, axis=0)
    return (field + extra.reshape(field.shape), motion)

def reference(positions, rhs, blob_owner, blob_row, blob_arm, body_inverse):
    body_ids = (blob_owner.reshape(-1) * BODY_DEV + blob_row.reshape(-1)).astype(jnp.int32)
    arms = blob_arm.reshape(3, -1)
    beta = jnp.sqrt(jnp.sum(rhs * rhs))
    basis = [rhs / beta]
    hessen = jnp.zeros((ITERS + 1, ITERS), jnp.float32)
    for column in range(ITERS):
        moved, unused = precondition(basis[column], arms, body_ids, body_inverse)
        fresh = mobility(moved, positions)
        inners = [jnp.sum(basis[row] * fresh) for row in range(column + 1)]
        for row in range(column + 1):
            fresh = fresh - inners[row] * basis[row]
            hessen = hessen.at[row, column].set(inners[row])
        length = jnp.sqrt(jnp.sum(fresh * fresh))
        hessen = hessen.at[column + 1, column].set(length)
        basis.append(fresh / length)
    normal_matrix = jnp.dot(hessen.T, hessen, precision=lax.Precision.HIGHEST)
    target = beta * hessen[0]
    factor = jnp.linalg.cholesky(normal_matrix)
    coeffs = jax.scipy.linalg.cho_solve((factor, True), target)
    combined = jnp.zeros_like(rhs)
    for column in range(ITERS):
        combined = combined + coeffs[column] * basis[column]
    blob_forces, body_motion = precondition(combined, arms, body_ids, body_inverse)
    return (blob_forces, body_motion)
```

```python
import functools
import math

import jax
import jax.numpy as jnp
from jax import lax
from jax.experimental import pallas as pl
from jax.experimental.pallas import tpu as pltpu
from jax.sharding import PartitionSpec as P

ITERS = 3
EPS2 = 0.04
KAPPA = 0.3
MESH = pl.DeviceIdType.MESH
F32 = jnp.float32
BF16 = jnp.bfloat16
CHUNK = 32


def split(value):
    high = value.astype(BF16).astype(F32)
    return high, value - high


def total_of(value):
    return jnp.sum(jnp.sum(value, axis=0, keepdims=True), axis=1, keepdims=True)


def kernel(
    ncell, nwide,
    pos_ref, rhs_ref, own_ref, row_ref, arm_ref, inv_ref,
    out_ref, motion_ref,
    ext0, wext, vext, movx, onehot, tpos, acc, bmat, sbuf, rbuf, mbuf, abuf,
    s_send, s_recv, a_send, a_recv, h_send, h_recv,
):
    ndev = ncell * nwide
    cell, wide = lax.axis_index("cell"), lax.axis_index("wide")
    me = cell * nwide + wide
    tiles, lanes = pos_ref.shape[1], pos_ref.shape[2]
    body_dev = inv_ref.shape[1] // 6
    rows = 6 * body_dev
    width = sbuf.shape[2]
    next_row = tiles + 2
    ext = 3 * next_row
    base = next_row + 1
    group = onehot.shape[2] // lanes
    factor = KAPPA / math.sqrt(9 * lanes)

    def peer_of(step):
        peer = lax.rem(me + step, ndev)
        return peer, (peer // nwide, lax.rem(peer, nwide))

    barrier = pltpu.get_barrier_semaphore()

    def greet(step, carry):
        pl.semaphore_signal(barrier, inc=1, device_id=peer_of(step)[1], device_id_type=MESH)
        return carry

    lax.fori_loop(1, ndev, greet, 0)

    own = pl.ds(base, tiles)
    for c in range(3):
        ext0[own, c, :] = pos_ref[c]
        ext0[own, 3 + c, :] = rhs_ref[c]
        ext0[own, 6 + c, :] = arm_ref[c]
    ext0[own, 9, :] = own_ref[...].astype(F32)
    ext0[own, 10, :] = row_ref[...].astype(F32)

    regions = [(dx, dy) for dx in (-1, 0, 1) for dy in (-1, 0, 1) if (dx, dy) != (0, 0)]

    def halo_copies(ref, slot):
        copies = []
        for k, (dx, dy) in enumerate(regions):
            first, count = {-1: (tiles - 1, 1), 0: (0, tiles), 1: (0, 1)}[dy]
            place = (1 + dx) * next_row + {-1: 0, 0: 1, 1: tiles + 1}[dy]
            copies.append(pltpu.make_async_remote_copy(
                src_ref=ref.at[pl.ds(base + first, count)],
                dst_ref=ref.at[pl.ds(place, count)],
                send_sem=h_send.at[slot, k],
                recv_sem=h_recv.at[slot, k],
                device_id=(lax.rem(cell - dx + ncell, ncell), lax.rem(wide - dy + nwide, nwide)),
                device_id_type=MESH,
            ))
        return copies

    def to_owner(step):
        peer, ids = peer_of(step)
        return pltpu.make_async_remote_copy(
            src_ref=sbuf.at[peer], dst_ref=rbuf.at[me],
            send_sem=s_send.at[step], recv_sem=s_recv.at[step],
            device_id=ids, device_id_type=MESH)

    def to_holder(step):
        peer, ids = peer_of(step)
        return pltpu.make_async_remote_copy(
            src_ref=mbuf.at[0], dst_ref=abuf.at[me],
            send_sem=a_send.at[step], recv_sem=a_recv.at[step],
            device_id=ids, device_id_type=MESH)

    def start_all(make):
        def body(step, carry):
            make(step).start()
            return carry
        lax.fori_loop(1, ndev, body, 0)

    def wait_all(make):
        def body(step, carry):
            make(step).wait()
            return carry
        lax.fori_loop(1, ndev, body, 0)

    arms = [arm_ref[c] for c in range(3)]
    row_flat = jnp.concatenate([row_ref[t : t + 1, :] for t in range(tiles)], axis=1)
    own_flat = jnp.concatenate([own_ref[t : t + 1, :] for t in range(tiles)], axis=1)
    nblob = tiles * lanes
    row_mask = lax.broadcasted_iota(jnp.int32, (body_dev, nblob), 0) == row_flat
    owner_hot = jnp.where(
        lax.broadcasted_iota(jnp.int32, (ndev, nblob), 0) == own_flat, 1.0, 0.0
    ).astype(BF16)
    lane_of = lax.broadcasted_iota(jnp.int32, (1, width), 1)

    def partial_sums(field, dots):
        sent = list(field) + [
            arms[1] * field[2] - arms[2] * field[1],
            arms[2] * field[0] - arms[0] * field[2],
            arms[0] * field[1] - arms[1] * field[0],
        ]
        result = jnp.zeros((ndev, width), F32)
        halves = [split(value) for value in sent]
        for part in range(2):
            pieces = []
            for c in range(6):
                value = halves[c][part]
                flat = jnp.concatenate([value[t : t + 1, :] for t in range(tiles)], axis=1)
                pieces.append(jnp.where(row_mask, flat, 0.0).astype(BF16))
            pieces.append(jnp.zeros((width - rows, nblob), BF16))
            spread = jnp.concatenate(pieces, axis=0)
            result = result + lax.dot_general(
                owner_hot, spread, (((1,), (1,)), ((), ())), preferred_element_type=F32)
        return result + scalars(dots)

    def scalars(dots):
        line = jnp.zeros((1, width), F32)
        for k, value in enumerate(dots):
            line = line + jnp.where(lane_of == rows + k, value, 0.0)
        return line

    def scatter_sums(values):
        sbuf[:, 0, :] = values
        rbuf[me] = sbuf[me]
        start_all(to_owner)

    def received(count):
        wait_all(to_owner)
        line = jnp.sum(rbuf[...], axis=0)
        return line, [
            jnp.sum(jnp.where(lane_of == rows + k, line, 0.0), axis=1, keepdims=True)
            for k in range(count)
        ]

    def give_motion(motion):
        mbuf[0] = motion
        abuf[me] = motion
        start_all(to_holder)

    first_field = [rhs_ref[c] for c in range(3)]
    squares = total_of(sum(f * f for f in first_field))
    first_sums = partial_sums(first_field, [squares])
    pl.semaphore_wait(barrier, ndev - 1)
    first_halo = halo_copies(ext0, 0)
    scatter_sums(first_sums)
    for copy in first_halo:
        copy.start()

    lane_row = lax.rem(lax.broadcasted_iota(jnp.int32, (body_dev, rows), 1), body_dev)
    diagonal = lane_row == lax.broadcasted_iota(jnp.int32, (body_dev, rows), 0)
    bmat[...] = jnp.zeros_like(bmat)
    for b in range(6):
        bmat[b * body_dev : (b + 1) * body_dev, 0:rows] = jnp.where(diagonal, inv_ref[b : b + 1, :], 0.0)

    def spread_target(t, carry):
        for c in range(3):
            line = pos_ref[c, pl.ds(t, 1), :]
            tpos[t, c] = jnp.broadcast_to(line, (lanes, lanes)).T
        return carry

    lax.fori_loop(0, tiles, spread_target, 0)

    def solve_motion(line):
        return jnp.dot(line, bmat[...], precision=lax.Precision.HIGHEST, preferred_element_type=F32)

    line, (beta2,) = received(1)
    beta = jnp.sqrt(beta2)
    motions = [solve_motion(line) / beta]
    give_motion(motions[0])
    for copy in first_halo:
        copy.wait()
    vext[0, :, 0:3, :] = ext0[:, 3:6, :] / beta[None]

    def make_hot(chunk, carry):
        for g in range(group):
            ids = ext0[chunk * group + g, 9:10, :].astype(jnp.int32)
            hot = jnp.where(lax.broadcasted_iota(jnp.int32, (ndev, lanes), 0) == ids, 1.0, 0.0).astype(BF16)
            onehot[chunk, 0:ndev, g * lanes : (g + 1) * lanes] = hot
            onehot[chunk, ndev : 2 * ndev, g * lanes : (g + 1) * lanes] = hot
        return carry

    lax.fori_loop(0, ext // group, make_hot, 0)

    def precondition(j):
        wait_all(to_holder)
        high, low = split(abuf[:, 0, :])
        table = jnp.concatenate([high, low], axis=0).T[0:rows].astype(BF16)

        def body(chunk, carry):
            found = jnp.dot(table, onehot[chunk], preferred_element_type=F32)
            for g in range(group):
                tile = chunk * group + g
                ids = ext0[tile, 10:11, :].astype(jnp.int32)
                mask = lax.broadcasted_iota(jnp.int32, (body_dev, lanes), 0) == ids
                m = []
                for a in range(6):
                    part = found[a * body_dev : (a + 1) * body_dev, g * lanes : (g + 1) * lanes]
                    m.append(jnp.sum(jnp.where(mask, part, 0.0), axis=0, keepdims=True))
                r = [ext0[tile, 6 + c : 7 + c, :] for c in range(3)]
                extra = [
                    m[0] + m[4] * r[2] - m[5] * r[1],
                    m[1] + m[5] * r[0] - m[3] * r[2],
                    m[2] + m[3] * r[1] - m[4] * r[0],
                ]
                for c in range(3):
                    movx[j, tile, c : c + 1, :] = vext[j, tile, c : c + 1, :] + extra[c]
            return carry

        lax.fori_loop(0, ext // group, body, 0)

    def mobility(j, slot):
        def body(t, carry):
            def part(q, carry):
                here = pl.ds(pl.multiple_of(q * CHUNK, CHUNK), CHUNK)
                target = [tpos[t, c, here, :] for c in range(3)]
                sums = [jnp.zeros((CHUNK, lanes), F32) for c in range(3)]
                for code in range(9):
                    dx, dy = code // 3 - 1, code % 3 - 1
                    tile = (1 + dx) * next_row + 1 + dy + t
                    shift = (float(dx), float(dy), 0.0)
                    sep = [target[c] - (ext0[tile, c : c + 1, :] + shift[c]) for c in range(3)]
                    force = [movx[j, tile, c : c + 1, :] for c in range(3)]
                    soft = sep[0] * sep[0] + sep[1] * sep[1] + (sep[2] * sep[2] + EPS2)
                    root = lax.rsqrt(soft)
                    cube = root * root * root
                    near = root + EPS2 * cube
                    along = cube * (sep[0] * force[0] + sep[1] * force[1] + sep[2] * force[2])
                    sums = [sums[c] + (near * force[c] + along * sep[c]) for c in range(3)]
                for c in range(3):
                    acc[c, here, :] = sums[c]
                return carry

            lax.fori_loop(0, lanes // CHUNK, part, 0)
            for c in range(3):
                line = jnp.sum(acc[c].T, axis=0, keepdims=True)
                wext[slot, base + t, c : c + 1, :] = movx[j, base + t, c : c + 1, :] + factor * line
            return carry

        lax.fori_loop(0, tiles, body, 0)

    hessen = []
    for j in range(ITERS):
        precondition(j)
        mobility(j, j)
        fresh = [wext[j, own, c, :] for c in range(3)]
        dots = []
        for i in range(j + 1):
            dots.append(total_of(sum(vext[i, own, c, :] * fresh[c] for c in range(3))))
        dots.append(total_of(sum(f * f for f in fresh)))
        last = j == ITERS - 1
        if not last:
            halo = halo_copies(wext.at[j], 1 + j)
            for copy in halo:
                copy.start()
            scatter_sums(partial_sums(fresh, dots))
        else:
            scatter_sums(jnp.broadcast_to(scalars(dots), (ndev, width)))
        line, values = received(j + 2)
        inners, whole = values[:-1], values[-1]
        squared = whole - sum(h * h for h in inners)
        length = jnp.sqrt(squared)
        hessen.append(inners + [length])
        if not last:
            motion = solve_motion(line)
            for i in range(j + 1):
                motion = motion - inners[i] * motions[i]
            motions.append(motion / length)
            give_motion(motions[-1])
            for copy in halo:
                copy.wait()
            value = wext[j]
            for i in range(j + 1):
                value = value - inners[i][None] * vext[i]
            vext[j + 1] = value / length[None]

    def entry(i, j):
        return hessen[j][i] if i <= j + 1 else None

    def normal(a, b):
        return sum(entry(i, a) * entry(i, b) for i in range(min(a, b) + 2))

    lower = [[None] * ITERS for _ in range(ITERS)]
    for a in range(ITERS):
        for b in range(a + 1):
            value = normal(a, b)
            for k in range(b):
                value = value - lower[a][k] * lower[b][k]
            lower[a][b] = jnp.sqrt(value) if a == b else value / lower[b][b]
    mid = []
    for a in range(ITERS):
        value = beta * entry(0, a)
        for k in range(a):
            value = value - lower[a][k] * mid[k]
        mid.append(value / lower[a][a])
    coeffs = [None] * ITERS
    for a in reversed(range(ITERS)):
        value = mid[a]
        for k in range(a + 1, ITERS):
            value = value - lower[k][a] * coeffs[k]
        coeffs[a] = value / lower[a][a]
    for c in range(3):
        out_ref[c] = sum(coeffs[j] * movx[j, own, c, :] for j in range(ITERS))
    motion_ref[...] = sum(coeffs[j] * motions[j] for j in range(ITERS))


def local(positions, rhs, blob_owner, blob_row, blob_arm, body_inverse):
    tiles, lanes = positions.shape[2], positions.shape[3]
    body_dev = body_inverse.shape[2]
    ncell, nwide = lax.axis_size("cell"), lax.axis_size("wide")
    ndev = ncell * nwide
    ext = 3 * (tiles + 2)
    group = 2 if ext % 2 == 0 else 1
    rows = 6 * body_dev
    width = -(-(rows + ITERS + 2) // 128) * 128
    inverse = jnp.transpose(body_inverse, (1, 0, 2)).reshape(6, rows)
    vmem = pl.BlockSpec(memory_space=pltpu.VMEM)
    forces, motion = pl.pallas_call(
        functools.partial(kernel, ncell, nwide),
        out_shape=(
            jax.ShapeDtypeStruct((3, tiles, lanes), F32),
            jax.ShapeDtypeStruct((1, width), F32),
        ),
        in_specs=[vmem] * 6,
        out_specs=(vmem, vmem),
        scratch_shapes=[
            pltpu.VMEM((ext, 16, lanes), F32),
            pltpu.VMEM((ITERS, ext, 4, lanes), F32),
            pltpu.VMEM((ITERS, ext, 4, lanes), F32),
            pltpu.VMEM((ITERS, ext, 4, lanes), F32),
            pltpu.VMEM((ext // group, 2 * ndev, group * lanes), BF16),
            pltpu.VMEM((tiles, 3, lanes, lanes), F32),
            pltpu.VMEM((3, lanes, lanes), F32),
            pltpu.VMEM((width, width), F32),
            pltpu.VMEM((ndev, 1, width), F32),
            pltpu.VMEM((ndev, 1, width), F32),
            pltpu.VMEM((1, 1, width), F32),
            pltpu.VMEM((ndev, 1, width), F32),
            pltpu.SemaphoreType.DMA((ndev,)),
            pltpu.SemaphoreType.DMA((ndev,)),
            pltpu.SemaphoreType.DMA((ndev,)),
            pltpu.SemaphoreType.DMA((ndev,)),
            pltpu.SemaphoreType.DMA((ITERS, 8)),
            pltpu.SemaphoreType.DMA((ITERS, 8)),
        ],
        compiler_params=pltpu.CompilerParams(
            collective_id=0, has_side_effects=True, vmem_limit_bytes=48 * 1024 * 1024
        ),
    )(
        positions[:, 0], rhs[:, 0], blob_owner.reshape(tiles, lanes),
        blob_row.reshape(tiles, lanes), blob_arm[:, 0], inverse,
    )
    return forces[:, None], motion[0, :rows].reshape(6, body_dev)


def solution(mesh):
    in_specs = (
        P(None, "cell", "wide", None),
        P(None, "cell", "wide", None),
        P("cell", "wide", None, None),
        P("cell", "wide", None),
        P(None, "cell", "wide", None),
        P(None, None, ("cell", "wide")),
    )
    out_specs = (P(None, "cell", "wide", None), P(None, ("cell", "wide")))
    return jax.shard_map(local, mesh=mesh, in_specs=in_specs, out_specs=out_specs, check_vma=False)
```

```python
import functools
import math

import jax
import jax.numpy as jnp
from jax import lax
from jax.experimental import pallas as pl
from jax.experimental.pallas import tpu as pltpu
from jax.sharding import PartitionSpec as P

ITERS = 3
EPS2 = 0.04
KAPPA = 0.3
MESH = pl.DeviceIdType.MESH
F32 = jnp.float32
BF16 = jnp.bfloat16
CHUNK = 32


def split(value):
    high = value.astype(BF16).astype(F32)
    return high, value - high


def total_of(value):
    return jnp.sum(jnp.sum(value, axis=0, keepdims=True), axis=1, keepdims=True)


def kernel(
    ncell, nwide,
    pos_ref, rhs_ref, own_ref, row_ref, arm_ref, inv_ref,
    out_ref, motion_ref,
    ext0, wext, vext, movx, onehot, tpos, acc, coef, bhigh, blow, sbuf, rbuf, mbuf, abuf,
    s_send, s_recv, a_send, a_recv, h_send, h_recv,
):
    ndev = ncell * nwide
    cell, wide = lax.axis_index("cell"), lax.axis_index("wide")
    me = cell * nwide + wide
    tiles, lanes = pos_ref.shape[1], pos_ref.shape[2]
    body_dev = inv_ref.shape[2]
    rows = 6 * body_dev
    width = sbuf.shape[2]
    next_row = tiles + 2
    ext = 3 * next_row
    base = next_row + 1
    group = onehot.shape[2] // lanes
    factor = KAPPA / math.sqrt(9 * lanes)

    cells = [cell] + [jnp.where(cell + a >= ncell, cell + a - ncell, cell + a) for a in range(1, ncell)]
    wides = [wide] + [jnp.where(wide + b >= nwide, wide + b - nwide, wide + b) for b in range(1, nwide)]
    far = sorted(range(ncell), key=lambda a: -min(a, ncell - a))
    peers = [(cells[a], wides[b]) for a in far for b in range(nwide) if (a, b) != (0, 0)]

    barrier = pltpu.get_barrier_semaphore()
    for ids in peers:
        pl.semaphore_signal(barrier, inc=1, device_id=ids, device_id_type=MESH)

    own = pl.ds(base, tiles)
    for c in range(3):
        ext0[own, c, :] = pos_ref[c]
        ext0[own, 3 + c, :] = rhs_ref[c]
        ext0[own, 6 + c, :] = arm_ref[c]
    ext0[own, 9, :] = own_ref[...].astype(F32)
    ext0[own, 10, :] = row_ref[...].astype(F32)

    regions = [(dx, dy) for dx in (-1, 0, 1) for dy in (-1, 0, 1) if (dx, dy) != (0, 0)]

    def halo_copies(ref, slot):
        copies = []
        for k, (dx, dy) in enumerate(regions):
            first, count = {-1: (tiles - 1, 1), 0: (0, tiles), 1: (0, 1)}[dy]
            place = (1 + dx) * next_row + {-1: 0, 0: 1, 1: tiles + 1}[dy]
            copies.append(pltpu.make_async_remote_copy(
                src_ref=ref.at[pl.ds(base + first, count)],
                dst_ref=ref.at[pl.ds(place, count)],
                send_sem=h_send.at[slot, k],
                recv_sem=h_recv.at[slot, k],
                device_id=(lax.rem(cell - dx + ncell, ncell), lax.rem(wide - dy + nwide, nwide)),
                device_id_type=MESH,
            ))
        return copies

    def start_sums():
        for ids in peers:
            pltpu.make_async_remote_copy(
                src_ref=sbuf.at[ids[0] * nwide + ids[1]], dst_ref=rbuf.at[me],
                send_sem=s_send, recv_sem=s_recv,
                device_id=ids, device_id_type=MESH).start()

    def wait_sums():
        whole = pl.ds(0, ndev - 1)
        pltpu.make_async_copy(rbuf.at[whole], rbuf.at[whole], s_recv).wait()
        pltpu.make_async_copy(sbuf.at[whole], sbuf.at[whole], s_send).wait()

    def start_motions():
        for ids in peers:
            pltpu.make_async_remote_copy(
                src_ref=mbuf.at[0], dst_ref=abuf.at[me],
                send_sem=a_send, recv_sem=a_recv,
                device_id=ids, device_id_type=MESH).start()

    def wait_motions():
        whole = pl.ds(0, ndev - 1)
        pltpu.make_async_copy(abuf.at[whole], abuf.at[whole], a_recv).wait()
        pltpu.make_async_copy(abuf.at[whole], abuf.at[whole], a_send).wait()

    arms = [arm_ref[c] for c in range(3)]
    row_flat = jnp.concatenate([row_ref[t : t + 1, :] for t in range(tiles)], axis=1)
    own_flat = jnp.concatenate([own_ref[t : t + 1, :] for t in range(tiles)], axis=1)
    nblob = tiles * lanes
    row_mask = lax.broadcasted_iota(jnp.int32, (body_dev, nblob), 0) == row_flat
    owner_hot = jnp.where(
        lax.broadcasted_iota(jnp.int32, (ndev, nblob), 0) == own_flat, 1.0, 0.0
    ).astype(BF16)
    lane_of = lax.broadcasted_iota(jnp.int32, (1, width), 1)

    def partial_sums(field, dots):
        sent = list(field) + [
            arms[1] * field[2] - arms[2] * field[1],
            arms[2] * field[0] - arms[0] * field[2],
            arms[0] * field[1] - arms[1] * field[0],
        ]
        result = jnp.zeros((ndev, width), F32)
        halves = [split(value) for value in sent]
        for part in range(2):
            pieces = []
            for c in range(6):
                value = halves[c][part]
                flat = jnp.concatenate([value[t : t + 1, :] for t in range(tiles)], axis=1)
                pieces.append(jnp.where(row_mask, flat, 0.0).astype(BF16))
            pieces.append(jnp.zeros((width - rows, nblob), BF16))
            spread = jnp.concatenate(pieces, axis=0)
            result = result + lax.dot_general(
                owner_hot, spread, (((1,), (1,)), ((), ())), preferred_element_type=F32)
        return result + scalars(dots)

    def scalars(dots):
        line = jnp.zeros((1, width), F32)
        for k, value in enumerate(dots):
            line = line + jnp.where(lane_of == rows + k, value, 0.0)
        return line

    def scatter_sums(values):
        sbuf[:, 0, :] = values
        rbuf[me] = sbuf[me]
        start_sums()

    def received(count):
        wait_sums()
        line = jnp.sum(rbuf[...], axis=0)
        return line, [
            jnp.sum(jnp.where(lane_of == rows + k, line, 0.0), axis=1, keepdims=True)
            for k in range(count)
        ]

    def give_motion(motion):
        mbuf[0] = motion
        abuf[me] = motion
        start_motions()

    first_field = [rhs_ref[c] for c in range(3)]
    squares = total_of(sum(f * f for f in first_field))
    first_sums = partial_sums(first_field, [squares])
    pl.semaphore_wait(barrier, ndev - 1)
    first_halo = halo_copies(ext0, 0)
    scatter_sums(first_sums)
    for copy in first_halo:
        copy.start()

    bhigh[...] = jnp.zeros_like(bhigh)
    blow[...] = jnp.zeros_like(blow)
    square = (body_dev, body_dev)
    diagonal = lax.broadcasted_iota(jnp.int32, square, 0) == lax.broadcasted_iota(jnp.int32, square, 1)
    for b in range(6):
        for a in range(6):
            high, low = split(inv_ref[a, b : b + 1, :])
            here = (slice(b * body_dev, (b + 1) * body_dev), slice(a * body_dev, (a + 1) * body_dev))
            bhigh[here] = jnp.where(diagonal, high, 0.0)
            blow[here] = jnp.where(diagonal, low, 0.0)

    def spread_target(t, carry):
        for c in range(3):
            line = pos_ref[c, pl.ds(t, 1), :]
            tpos[t, c] = jnp.broadcast_to(line, (lanes, lanes)).T
        return carry

    lax.fori_loop(0, tiles, spread_target, 0)

    def coefficients(t, carry):
        def part(q, carry):
            here = pl.ds(pl.multiple_of(q * CHUNK, CHUNK), CHUNK)
            target = [tpos[t, c, here, :] for c in range(3)]
            for code in range(9):
                dx, dy = code // 3 - 1, code % 3 - 1
                tile = (1 + dx) * next_row + 1 + dy + t
                shift = (float(dx), float(dy), 0.0)
                sep = [target[c] - (ext0[tile, c : c + 1, :] + shift[c]) for c in range(3)]
                soft = sep[0] * sep[0] + sep[1] * sep[1] + (sep[2] * sep[2] + EPS2)
                root = lax.rsqrt(soft)
                twice = root * root
                coef[t * 9 + code, 3, here, :] = root + EPS2 * (twice * root)
                scale = twice * lax.rsqrt(root)
                for c in range(3):
                    coef[t * 9 + code, c, here, :] = scale * sep[c]
            return carry

        return lax.fori_loop(0, lanes // CHUNK, part, carry)

    def solve_motion(line):
        high, low = split(line)
        both = jnp.concatenate([high, low], axis=0).astype(BF16)
        one = jnp.dot(both, bhigh[...].astype(BF16), preferred_element_type=F32)
        two = jnp.dot(both, blow[...].astype(BF16), preferred_element_type=F32)
        return one[0:1] + one[1:2] + two[0:1]

    for copy in first_halo:
        copy.wait()
    lax.fori_loop(0, tiles // 2, coefficients, 0)
    line, (beta2,) = received(1)
    beta = jnp.sqrt(beta2)
    motions = [solve_motion(line) / beta]
    give_motion(motions[0])
    vext[0, :, 0:3, :] = ext0[:, 3:6, :] / beta[None]

    def make_hot(chunk, carry):
        for g in range(group):
            ids = ext0[chunk * group + g, 9:10, :].astype(jnp.int32)
            hot = jnp.where(lax.broadcasted_iota(jnp.int32, (ndev, lanes), 0) == ids, 1.0, 0.0).astype(BF16)
            onehot[chunk, 0:ndev, g * lanes : (g + 1) * lanes] = hot
            onehot[chunk, ndev : 2 * ndev, g * lanes : (g + 1) * lanes] = hot
        return carry

    lax.fori_loop(0, ext // group, make_hot, 0)
    lax.fori_loop(tiles // 2, tiles, coefficients, 0)

    def precondition(j):
        wait_motions()
        high, low = split(abuf[:, 0, :])
        table = jnp.concatenate([high, low], axis=0).T[0:rows].astype(BF16)

        def body(chunk, carry):
            found = jnp.dot(table, onehot[chunk], preferred_element_type=F32)
            for g in range(group):
                tile = chunk * group + g
                ids = ext0[tile, 10:11, :].astype(jnp.int32)
                mask = lax.broadcasted_iota(jnp.int32, (body_dev, lanes), 0) == ids
                m = []
                for a in range(6):
                    part = found[a * body_dev : (a + 1) * body_dev, g * lanes : (g + 1) * lanes]
                    m.append(jnp.sum(jnp.where(mask, part, 0.0), axis=0, keepdims=True))
                r = [ext0[tile, 6 + c : 7 + c, :] for c in range(3)]
                extra = [
                    m[0] + m[4] * r[2] - m[5] * r[1],
                    m[1] + m[5] * r[0] - m[3] * r[2],
                    m[2] + m[3] * r[1] - m[4] * r[0],
                ]
                for c in range(3):
                    movx[j, tile, c : c + 1, :] = vext[j, tile, c : c + 1, :] + extra[c]
            return carry

        lax.fori_loop(0, ext // group, body, 0)

    def mobility(j, slot):
        def body(t, carry):
            def part(q, carry):
                here = pl.ds(pl.multiple_of(q * CHUNK, CHUNK), CHUNK)
                sums = [jnp.zeros((CHUNK, lanes), F32) for c in range(3)]
                for code in range(9):
                    tile = (code // 3) * next_row + code % 3 + t
                    near = coef[t * 9 + code, 3, here, :]
                    unit = [coef[t * 9 + code, c, here, :] for c in range(3)]
                    force = [movx[j, tile, c : c + 1, :] for c in range(3)]
                    along = unit[0] * force[0] + unit[1] * force[1] + unit[2] * force[2]
                    sums = [sums[c] + (near * force[c] + along * unit[c]) for c in range(3)]
                for c in range(3):
                    acc[c, here, :] = sums[c]
                return carry

            lax.fori_loop(0, lanes // CHUNK, part, 0)
            for c in range(3):
                line = jnp.sum(acc[c].T, axis=0, keepdims=True)
                wext[slot, base + t, c : c + 1, :] = movx[j, base + t, c : c + 1, :] + factor * line
            return carry

        lax.fori_loop(0, tiles, body, 0)

    hessen = []
    for j in range(ITERS):
        precondition(j)
        mobility(j, j)
        fresh = [wext[j, own, c, :] for c in range(3)]
        dots = []
        for i in range(j + 1):
            dots.append(total_of(sum(vext[i, own, c, :] * fresh[c] for c in range(3))))
        dots.append(total_of(sum(f * f for f in fresh)))
        last = j == ITERS - 1
        if not last:
            halo = halo_copies(wext.at[j], 1 + j)
            for copy in halo:
                copy.start()
            scatter_sums(partial_sums(fresh, dots))
        else:
            scatter_sums(jnp.broadcast_to(scalars(dots), (ndev, width)))
        line, values = received(j + 2)
        inners, whole = values[:-1], values[-1]
        squared = whole - sum(h * h for h in inners)
        length = jnp.sqrt(squared)
        hessen.append(inners + [length])
        if not last:
            motion = solve_motion(line)
            for i in range(j + 1):
                motion = motion - inners[i] * motions[i]
            motions.append(motion / length)
            give_motion(motions[-1])
            for copy in halo:
                copy.wait()
            value = wext[j]
            for i in range(j + 1):
                value = value - inners[i][None] * vext[i]
            vext[j + 1] = value / length[None]

    def entry(i, j):
        return hessen[j][i] if i <= j + 1 else None

    def normal(a, b):
        return sum(entry(i, a) * entry(i, b) for i in range(min(a, b) + 2))

    lower = [[None] * ITERS for _ in range(ITERS)]
    for a in range(ITERS):
        for b in range(a + 1):
            value = normal(a, b)
            for k in range(b):
                value = value - lower[a][k] * lower[b][k]
            lower[a][b] = jnp.sqrt(value) if a == b else value / lower[b][b]
    mid = []
    for a in range(ITERS):
        value = beta * entry(0, a)
        for k in range(a):
            value = value - lower[a][k] * mid[k]
        mid.append(value / lower[a][a])
    coeffs = [None] * ITERS
    for a in reversed(range(ITERS)):
        value = mid[a]
        for k in range(a + 1, ITERS):
            value = value - lower[k][a] * coeffs[k]
        coeffs[a] = value / lower[a][a]
    for c in range(3):
        out_ref[c] = sum(coeffs[j] * movx[j, own, c, :] for j in range(ITERS))
    motion = sum(coeffs[j] * motions[j] for j in range(ITERS))
    for a in range(6):
        motion_ref[a : a + 1, :] = motion[:, a * body_dev : (a + 1) * body_dev]


def local(positions, rhs, blob_owner, blob_row, blob_arm, body_inverse):
    tiles, lanes = positions.shape[2], positions.shape[3]
    body_dev = body_inverse.shape[2]
    ncell, nwide = lax.axis_size("cell"), lax.axis_size("wide")
    ndev = ncell * nwide
    ext = 3 * (tiles + 2)
    group = 6 if ext % 6 == 0 else 3
    rows = 6 * body_dev
    width = -(-(rows + ITERS + 2) // 128) * 128
    vmem = pl.BlockSpec(memory_space=pltpu.VMEM)
    forces, motion = pl.pallas_call(
        functools.partial(kernel, ncell, nwide),
        out_shape=(
            jax.ShapeDtypeStruct((3, tiles, lanes), F32),
            jax.ShapeDtypeStruct((6, body_dev), F32),
        ),
        in_specs=[vmem] * 6,
        out_specs=(vmem, vmem),
        scratch_shapes=[
            pltpu.VMEM((ext, 16, lanes), F32),
            pltpu.VMEM((ITERS, ext, 4, lanes), F32),
            pltpu.VMEM((ITERS, ext, 4, lanes), F32),
            pltpu.VMEM((ITERS, ext, 4, lanes), F32),
            pltpu.VMEM((ext // group, 2 * ndev, group * lanes), BF16),
            pltpu.VMEM((tiles, 3, lanes, lanes), F32),
            pltpu.VMEM((3, lanes, lanes), F32),
            pltpu.VMEM((9 * tiles, 4, lanes, lanes), F32),
            pltpu.VMEM((width, width), F32),
            pltpu.VMEM((width, width), F32),
            pltpu.VMEM((ndev, 1, width), F32),
            pltpu.VMEM((ndev, 1, width), F32),
            pltpu.VMEM((1, 1, width), F32),
            pltpu.VMEM((ndev, 1, width), F32),
            pltpu.SemaphoreType.DMA,
            pltpu.SemaphoreType.DMA,
            pltpu.SemaphoreType.DMA,
            pltpu.SemaphoreType.DMA,
            pltpu.SemaphoreType.DMA((ITERS, 8)),
            pltpu.SemaphoreType.DMA((ITERS, 8)),
        ],
        compiler_params=pltpu.CompilerParams(
            collective_id=0, has_side_effects=True, vmem_limit_bytes=48 * 1024 * 1024
        ),
    )(
        positions[:, 0], rhs[:, 0], blob_owner.reshape(tiles, lanes),
        blob_row.reshape(tiles, lanes), blob_arm[:, 0], body_inverse,
    )
    return forces[:, None], motion


def solution(mesh):
    in_specs = (
        P(None, "cell", "wide", None),
        P(None, "cell", "wide", None),
        P("cell", "wide", None, None),
        P("cell", "wide", None),
        P(None, "cell", "wide", None),
        P(None, None, ("cell", "wide")),
    )
    out_specs = (P(None, "cell", "wide", None), P(None, ("cell", "wide")))
    return jax.shard_map(local, mesh=mesh, in_specs=in_specs, out_specs=out_specs, check_vma=False)
```

```python
import functools
import math

import jax
import jax.numpy as jnp
from jax import lax
from jax.experimental import pallas as pl
from jax.experimental.pallas import tpu as pltpu
from jax.sharding import PartitionSpec as P

ITERS = 3
EPS2 = 0.04
KAPPA = 0.3
MESH = pl.DeviceIdType.MESH
F32 = jnp.float32
BF16 = jnp.bfloat16
CHUNK = 32


def split(value):
    high = value.astype(BF16).astype(F32)
    return high, value - high


def total_of(value):
    return jnp.sum(jnp.sum(value, axis=0, keepdims=True), axis=1, keepdims=True)


def kernel(
    ncell, nwide,
    pos_ref, rhs_ref, own_ref, row_ref, arm_ref, inv_ref,
    out_ref, motion_ref,
    ext0, wext, vext, movx, onehot, tpos, acc, coef, bhigh, blow, sbuf, rbuf, mbuf, abuf,
    s_send, s_recv, a_send, a_recv, h_send, h_recv,
):
    ndev = ncell * nwide
    cell, wide = lax.axis_index("cell"), lax.axis_index("wide")
    me = cell * nwide + wide
    tiles, lanes = pos_ref.shape[1], pos_ref.shape[2]
    body_dev = inv_ref.shape[2]
    rows = 6 * body_dev
    width = sbuf.shape[2]
    next_row = tiles + 2
    ext = 3 * next_row
    base = next_row + 1
    group = onehot.shape[2] // lanes
    factor = KAPPA / math.sqrt(9 * lanes)

    cells = [cell] + [jnp.where(cell + a >= ncell, cell + a - ncell, cell + a) for a in range(1, ncell)]
    wides = [wide] + [jnp.where(wide + b >= nwide, wide + b - nwide, wide + b) for b in range(1, nwide)]
    far = sorted(range(ncell), key=lambda a: -min(a, ncell - a))
    peers = [(cells[a], wides[b]) for a in far for b in range(nwide) if (a, b) != (0, 0)]

    barrier = pltpu.get_barrier_semaphore()
    for ids in peers:
        pl.semaphore_signal(barrier, inc=1, device_id=ids, device_id_type=MESH)

    own = pl.ds(base, tiles)
    for c in range(3):
        ext0[own, c, :] = pos_ref[c]
        ext0[own, 3 + c, :] = rhs_ref[c]
        ext0[own, 6 + c, :] = arm_ref[c]
    ext0[own, 9, :] = own_ref[...].astype(F32)
    ext0[own, 10, :] = row_ref[...].astype(F32)

    regions = [(dx, dy) for dx in (-1, 0, 1) for dy in (-1, 0, 1) if (dx, dy) != (0, 0)]

    def halo_copies(ref, slot):
        copies = []
        for k, (dx, dy) in enumerate(regions):
            first, count = {-1: (tiles - 1, 1), 0: (0, tiles), 1: (0, 1)}[dy]
            place = (1 + dx) * next_row + {-1: 0, 0: 1, 1: tiles + 1}[dy]
            copies.append(pltpu.make_async_remote_copy(
                src_ref=ref.at[pl.ds(base + first, count)],
                dst_ref=ref.at[pl.ds(place, count)],
                send_sem=h_send.at[slot, k],
                recv_sem=h_recv.at[slot, k],
                device_id=(lax.rem(cell - dx + ncell, ncell), lax.rem(wide - dy + nwide, nwide)),
                device_id_type=MESH,
            ))
        return copies

    def start_sums():
        for ids in peers:
            pltpu.make_async_remote_copy(
                src_ref=sbuf.at[ids[0] * nwide + ids[1]], dst_ref=rbuf.at[me],
                send_sem=s_send, recv_sem=s_recv,
                device_id=ids, device_id_type=MESH).start()

    def wait_sums():
        whole = pl.ds(0, ndev - 1)
        pltpu.make_async_copy(rbuf.at[whole], rbuf.at[whole], s_recv).wait()
        pltpu.make_async_copy(sbuf.at[whole], sbuf.at[whole], s_send).wait()

    def start_motions():
        for ids in peers:
            pltpu.make_async_remote_copy(
                src_ref=mbuf.at[0], dst_ref=abuf.at[me],
                send_sem=a_send, recv_sem=a_recv,
                device_id=ids, device_id_type=MESH).start()

    def wait_motions():
        whole = pl.ds(0, ndev - 1)
        pltpu.make_async_copy(abuf.at[whole], abuf.at[whole], a_recv).wait()
        pltpu.make_async_copy(abuf.at[whole], abuf.at[whole], a_send).wait()

    arms = [arm_ref[c] for c in range(3)]
    row_flat = jnp.concatenate([row_ref[t : t + 1, :] for t in range(tiles)], axis=1)
    own_flat = jnp.concatenate([own_ref[t : t + 1, :] for t in range(tiles)], axis=1)
    nblob = tiles * lanes
    row_mask = lax.broadcasted_iota(jnp.int32, (body_dev, nblob), 0) == row_flat
    owner_hot = jnp.where(
        lax.broadcasted_iota(jnp.int32, (ndev, nblob), 0) == own_flat, 1.0, 0.0
    ).astype(BF16)
    lane_of = lax.broadcasted_iota(jnp.int32, (1, width), 1)

    def partial_sums(field, dots):
        sent = list(field) + [
            arms[1] * field[2] - arms[2] * field[1],
            arms[2] * field[0] - arms[0] * field[2],
            arms[0] * field[1] - arms[1] * field[0],
        ]
        result = jnp.zeros((ndev, width), F32)
        halves = [split(value) for value in sent]
        for part in range(2):
            pieces = []
            for c in range(6):
                value = halves[c][part]
                flat = jnp.concatenate([value[t : t + 1, :] for t in range(tiles)], axis=1)
                pieces.append(jnp.where(row_mask, flat, 0.0).astype(BF16))
            pieces.append(jnp.zeros((width - rows, nblob), BF16))
            spread = jnp.concatenate(pieces, axis=0)
            result = result + lax.dot_general(
                owner_hot, spread, (((1,), (1,)), ((), ())), preferred_element_type=F32)
        return result + scalars(dots)

    def scalars(dots):
        line = jnp.zeros((1, width), F32)
        for k, value in enumerate(dots):
            line = line + jnp.where(lane_of == rows + k, value, 0.0)
        return line

    def scatter_sums(values):
        sbuf[:, 0, :] = values
        rbuf[me] = sbuf[me]
        start_sums()

    def received(count):
        wait_sums()
        line = jnp.sum(rbuf[...], axis=0)
        return line, [
            jnp.sum(jnp.where(lane_of == rows + k, line, 0.0), axis=1, keepdims=True)
            for k in range(count)
        ]

    def give_motion(motion):
        mbuf[0] = motion
        abuf[me] = motion
        start_motions()

    first_field = [rhs_ref[c] for c in range(3)]
    squares = total_of(sum(f * f for f in first_field))
    first_sums = partial_sums(first_field, [squares])
    pl.semaphore_wait(barrier, ndev - 1)
    first_halo = halo_copies(ext0, 0)
    scatter_sums(first_sums)
    for copy in first_halo:
        copy.start()

    bhigh[...] = jnp.zeros_like(bhigh)
    blow[...] = jnp.zeros_like(blow)
    square = (body_dev, body_dev)
    diagonal = lax.broadcasted_iota(jnp.int32, square, 0) == lax.broadcasted_iota(jnp.int32, square, 1)
    for b in range(6):
        for a in range(6):
            high, low = split(inv_ref[a, b : b + 1, :])
            here = (slice(b * body_dev, (b + 1) * body_dev), slice(a * body_dev, (a + 1) * body_dev))
            bhigh[here] = jnp.where(diagonal, high, 0.0)
            blow[here] = jnp.where(diagonal, low, 0.0)

    def spread_target(t, carry):
        for c in range(3):
            line = pos_ref[c, pl.ds(t, 1), :]
            tpos[t, c] = jnp.broadcast_to(line, (lanes, lanes)).T
        return carry

    lax.fori_loop(0, tiles, spread_target, 0)

    def coefficients(t, carry):
        def part(q, carry):
            here = pl.ds(pl.multiple_of(q * CHUNK, CHUNK), CHUNK)
            target = [tpos[t, c, here, :] for c in range(3)]
            for code in range(9):
                dx, dy = code // 3 - 1, code % 3 - 1
                tile = (1 + dx) * next_row + 1 + dy + t
                shift = (float(dx), float(dy), 0.0)
                sep = [target[c] - (ext0[tile, c : c + 1, :] + shift[c]) for c in range(3)]
                soft = sep[0] * sep[0] + sep[1] * sep[1] + (sep[2] * sep[2] + EPS2)
                root = lax.rsqrt(soft)
                twice = root * root
                coef[t * 9 + code, 3, here, :] = root + EPS2 * (twice * root)
                scale = twice * lax.rsqrt(root)
                for c in range(3):
                    coef[t * 9 + code, c, here, :] = scale * sep[c]
            return carry

        return lax.fori_loop(0, lanes // CHUNK, part, carry)

    def solve_motion(line):
        high, low = split(line)
        both = jnp.concatenate([high, low], axis=0).astype(BF16)
        one = jnp.dot(both, bhigh[...].astype(BF16), preferred_element_type=F32)
        two = jnp.dot(both, blow[...].astype(BF16), preferred_element_type=F32)
        return one[0:1] + one[1:2] + two[0:1]

    for copy in first_halo:
        copy.wait()
    line, (beta2,) = received(1)
    beta = jnp.sqrt(beta2)
    motions = [solve_motion(line) / beta]
    give_motion(motions[0])
    vext[0, :, 0:3, :] = ext0[:, 3:6, :] / beta[None]

    def make_hot(chunk, carry):
        for g in range(group):
            ids = ext0[chunk * group + g, 9:10, :].astype(jnp.int32)
            hot = jnp.where(lax.broadcasted_iota(jnp.int32, (ndev, lanes), 0) == ids, 1.0, 0.0).astype(BF16)
            onehot[chunk, 0:ndev, g * lanes : (g + 1) * lanes] = hot
            onehot[chunk, ndev : 2 * ndev, g * lanes : (g + 1) * lanes] = hot
        return carry

    lax.fori_loop(0, ext // group, make_hot, 0)
    lax.fori_loop(0, tiles, coefficients, 0)

    def precondition(j):
        wait_motions()
        high, low = split(abuf[:, 0, :])
        table = jnp.concatenate([high, low], axis=0).T[0:rows].astype(BF16)

        def body(chunk, carry):
            found = jnp.dot(table, onehot[chunk], preferred_element_type=F32)
            for g in range(group):
                tile = chunk * group + g
                ids = ext0[tile, 10:11, :].astype(jnp.int32)
                mask = lax.broadcasted_iota(jnp.int32, (body_dev, lanes), 0) == ids
                m = []
                for a in range(6):
                    part = found[a * body_dev : (a + 1) * body_dev, g * lanes : (g + 1) * lanes]
                    m.append(jnp.sum(jnp.where(mask, part, 0.0), axis=0, keepdims=True))
                r = [ext0[tile, 6 + c : 7 + c, :] for c in range(3)]
                extra = [
                    m[0] + m[4] * r[2] - m[5] * r[1],
                    m[1] + m[5] * r[0] - m[3] * r[2],
                    m[2] + m[3] * r[1] - m[4] * r[0],
                ]
                for c in range(3):
                    movx[j, tile, c : c + 1, :] = vext[j, tile, c : c + 1, :] + extra[c]
            return carry

        for chunk in range(ext // group):
            body(chunk, 0)

    def mobility(j, slot):
        def body(t, carry):
            def part(q, carry):
                here = slice(q * CHUNK, (q + 1) * CHUNK)
                sums = [jnp.zeros((CHUNK, lanes), F32) for c in range(3)]
                for code in range(9):
                    tile = (code // 3) * next_row + code % 3 + t
                    near = coef[t * 9 + code, 3, here, :]
                    unit = [coef[t * 9 + code, c, here, :] for c in range(3)]
                    force = [movx[j, tile, c : c + 1, :] for c in range(3)]
                    along = unit[0] * force[0] + unit[1] * force[1] + unit[2] * force[2]
                    sums = [sums[c] + (near * force[c] + along * unit[c]) for c in range(3)]
                for c in range(3):
                    acc[3 * t + c, here, :] = sums[c]
                return carry

            for q in range(lanes // CHUNK):
                part(q, 0)
            return carry

        lax.fori_loop(0, tiles, body, 0)
        for t in range(tiles):
            for c in range(3):
                line = jnp.sum(acc[3 * t + c].T, axis=0, keepdims=True)
                wext[slot, base + t, c : c + 1, :] = movx[j, base + t, c : c + 1, :] + factor * line

    hessen = []
    for j in range(ITERS):
        precondition(j)
        mobility(j, j)
        fresh = [wext[j, own, c, :] for c in range(3)]
        dots = []
        for i in range(j + 1):
            dots.append(total_of(sum(vext[i, own, c, :] * fresh[c] for c in range(3))))
        dots.append(total_of(sum(f * f for f in fresh)))
        last = j == ITERS - 1
        if not last:
            halo = halo_copies(wext.at[j], 1 + j)
            for copy in halo:
                copy.start()
            scatter_sums(partial_sums(fresh, dots))
        else:
            scatter_sums(jnp.broadcast_to(scalars(dots), (ndev, width)))
        line, values = received(j + 2)
        inners, whole = values[:-1], values[-1]
        squared = whole - sum(h * h for h in inners)
        length = jnp.sqrt(squared)
        hessen.append(inners + [length])
        if not last:
            motion = solve_motion(line)
            for i in range(j + 1):
                motion = motion - inners[i] * motions[i]
            motions.append(motion / length)
            give_motion(motions[-1])
            for copy in halo:
                copy.wait()
            value = wext[j]
            for i in range(j + 1):
                value = value - inners[i][None] * vext[i]
            vext[j + 1] = value / length[None]

    def entry(i, j):
        return hessen[j][i] if i <= j + 1 else None

    def normal(a, b):
        return sum(entry(i, a) * entry(i, b) for i in range(min(a, b) + 2))

    lower = [[None] * ITERS for _ in range(ITERS)]
    for a in range(ITERS):
        for b in range(a + 1):
            value = normal(a, b)
            for k in range(b):
                value = value - lower[a][k] * lower[b][k]
            lower[a][b] = jnp.sqrt(value) if a == b else value / lower[b][b]
    mid = []
    for a in range(ITERS):
        value = beta * entry(0, a)
        for k in range(a):
            value = value - lower[a][k] * mid[k]
        mid.append(value / lower[a][a])
    coeffs = [None] * ITERS
    for a in reversed(range(ITERS)):
        value = mid[a]
        for k in range(a + 1, ITERS):
            value = value - lower[k][a] * coeffs[k]
        coeffs[a] = value / lower[a][a]
    for c in range(3):
        out_ref[c] = sum(coeffs[j] * movx[j, own, c, :] for j in range(ITERS))
    motion = sum(coeffs[j] * motions[j] for j in range(ITERS))
    for a in range(6):
        motion_ref[a : a + 1, :] = motion[:, a * body_dev : (a + 1) * body_dev]


def local(positions, rhs, blob_owner, blob_row, blob_arm, body_inverse):
    tiles, lanes = positions.shape[2], positions.shape[3]
    body_dev = body_inverse.shape[2]
    ncell, nwide = lax.axis_size("cell"), lax.axis_size("wide")
    ndev = ncell * nwide
    ext = 3 * (tiles + 2)
    group = 6 if ext % 6 == 0 else 3
    rows = 6 * body_dev
    width = -(-(rows + ITERS + 2) // 128) * 128
    vmem = pl.BlockSpec(memory_space=pltpu.VMEM)
    forces, motion = pl.pallas_call(
        functools.partial(kernel, ncell, nwide),
        out_shape=(
            jax.ShapeDtypeStruct((3, tiles, lanes), F32),
            jax.ShapeDtypeStruct((6, body_dev), F32),
        ),
        in_specs=[vmem] * 6,
        out_specs=(vmem, vmem),
        scratch_shapes=[
            pltpu.VMEM((ext, 16, lanes), F32),
            pltpu.VMEM((ITERS, ext, 4, lanes), F32),
            pltpu.VMEM((ITERS, ext, 4, lanes), F32),
            pltpu.VMEM((ITERS, ext, 4, lanes), F32),
            pltpu.VMEM((ext // group, 2 * ndev, group * lanes), BF16),
            pltpu.VMEM((tiles, 3, lanes, lanes), F32),
            pltpu.VMEM((3 * tiles, lanes, lanes), F32),
            pltpu.VMEM((9 * tiles, 4, lanes, lanes), F32),
            pltpu.VMEM((width, width), F32),
            pltpu.VMEM((width, width), F32),
            pltpu.VMEM((ndev, 1, width), F32),
            pltpu.VMEM((ndev, 1, width), F32),
            pltpu.VMEM((1, 1, width), F32),
            pltpu.VMEM((ndev, 1, width), F32),
            pltpu.SemaphoreType.DMA,
            pltpu.SemaphoreType.DMA,
            pltpu.SemaphoreType.DMA,
            pltpu.SemaphoreType.DMA,
            pltpu.SemaphoreType.DMA((ITERS, 8)),
            pltpu.SemaphoreType.DMA((ITERS, 8)),
        ],
        compiler_params=pltpu.CompilerParams(
            collective_id=0, has_side_effects=True, vmem_limit_bytes=48 * 1024 * 1024
        ),
    )(
        positions[:, 0], rhs[:, 0], blob_owner.reshape(tiles, lanes),
        blob_row.reshape(tiles, lanes), blob_arm[:, 0], body_inverse,
    )
    return forces[:, None], motion


def solution(mesh):
    in_specs = (
        P(None, "cell", "wide", None),
        P(None, "cell", "wide", None),
        P("cell", "wide", None, None),
        P("cell", "wide", None),
        P(None, "cell", "wide", None),
        P(None, None, ("cell", "wide")),
    )
    out_specs = (P(None, "cell", "wide", None), P(None, ("cell", "wide")))
    return jax.shard_map(local, mesh=mesh, in_specs=in_specs, out_specs=out_specs, check_vma=False)
```
